32 devices in a mesh: group: 2 (over y), seq: 4 (over z), head: 2 (over x), sub: 2 (over core).
Axes of the slice: x: 2, y: 2, z: 4, core: 2. Of those that a mesh axis runs over, the one named last changes fastest.
Arguments:
- queries: bfloat16 [4, 32, 128], P(('group', 'sub'), 'head'), parts along dimension 0, may hold values from -8 to 8
- lengths: int32 [4], P(('group', 'sub')), parts along dimension 0, may hold values from 1 to 192, 256 in all
- k_cache: bfloat16 [65536, 8, 128], P(('group', 'seq', 'sub'), 'head'), parts along dimension 0, may hold values from -12 to 12
- v_cache: bfloat16 [65536, 8, 128], P(('group', 'seq', 'sub'), 'head'), parts along dimension 0, may hold values from -6 to 6
Outputs:
- attended: bfloat16 [4, 32, 128], P('group', ('head', 'sub')), parts along dimension 0
The draws below stay inside these ranges and needn't reach their ends.
There are 2 independent parts, one for each index of `group`. The reference program is written for one: setup_inputs(seed, part) draws one part's arguments, and reference() takes and returns one part's arrays. A program takes and returns all parts, laid end to end along the dimension named above; each array names one. Nothing has to cross between parts.
Inputs may be any that keep to these rules, and one draw needn't show every extreme that they name: The lengths sum to exactly 256, and some request has exactly 192 pages.
All inputs are finite; a program needn't handle non-finite values. No bound on the sum of `lengths` on one device may be relied on, other than what follows from the above.
Results may differ from the reference program's by a relative error of at most 0.0044.
Values may be sent and summed in bfloat16 or wider, within the bound.
A program may use at most 64 MiB of HBM per device.

```python
import math
import jax
import jax.numpy as jnp
import numpy as np
from jax import lax

QH = 32
KVH = 8
HD = 128
PAGE = 128
R = 2
TOTAL_PAGES = 256
TOKENS = 32768
MOST = 192


def draw_queries(key, part):
    noise = jnp.clip(jax.random.normal(jax.random.fold_in(key, 11), (R, QH, HD), jnp.float32), -6.0, 6.0)
    values = noise
    return values.astype(jnp.bfloat16)


def draw_k_cache(key, part):
    noise = jnp.clip(jax.random.normal(jax.random.fold_in(key, 17), (TOKENS, KVH, HD), jnp.float32), -6.0, 6.0)
    values = noise
    return values.astype(jnp.bfloat16)


def shard_levels(own_key, dims, shards, low, high):
    factor_of = 1.0
    for dim, blocks in shards:
        draws = jax.random.uniform(jax.random.fold_in(jax.random.fold_in(own_key, 6), dim), (blocks,), jnp.float32, low / len(shards), high / len(shards))
        factor_of = factor_of * jnp.repeat(jnp.exp(draws), dims[dim] // blocks).reshape((-1,) + (1,) * (len(dims) - 1 - dim))
    return factor_of


def split_up(count, total, reach, skew):
    portions = [(1 << 20) // math.isqrt(grade ** skew) + 1 for grade in range(2, count + 1)]
    surplus, holding = total - reach - (count - 1), [1] * (count - 1)
    while surplus > 0:
        free = [i for i in range(count - 1) if holding[i] < reach]
        mass, remaining = sum([portions[i] for i in free]), surplus
        for i in free:
            addition = min(reach - holding[i], max(1, remaining * portions[i] // mass), surplus)
            holding[i] = holding[i] + addition
            surplus = surplus - addition
    return np.array([reach] + holding)


def uneven_parts(rng, number_of, total, reach, slope):
    if number_of == 2:
        one = jax.random.randint(rng, (), max(1, total - reach), min(reach, total - 1) + 1)
        return jnp.stack([one, total - one])
    tallies = jnp.asarray(split_up(number_of, total, reach, slope), jnp.int32)
    twos = (number_of - 1) // 2
    source_of, receiver = tallies[1:1 + 2 * twos:2], tallies[2:2 + 2 * twos:2]
    slack = jnp.minimum(source_of - 1, reach - receiver)
    moved = jax.random.randint(jax.random.fold_in(rng, 1), (twos,), 0, 1 << 20) % (slack + 1)
    tallies = tallies.at[1:1 + 2 * twos:2].set(source_of - moved).at[2:2 + 2 * twos:2].set(receiver + moved)
    return tallies[jax.random.permutation(jax.random.fold_in(rng, 2), number_of)]


def centred(key, dims, deviation, most, shards=(), kind=jnp.bfloat16):
    array = deviation * jax.random.normal(key, dims, jnp.float32)
    if shards:
        array = array * shard_levels(key, dims, shards, -0.22, 0.18)
    return jnp.clip(array, -most, most).astype(kind)


def setup_inputs(seed: int = 0, part: int = 0) -> dict:
    key_of = jax.random.split(jax.random.key(seed), 5)
    part_keys = jax.random.split(jax.random.fold_in(key_of[4], part), 5)
    queries = draw_queries(jax.random.fold_in(jax.random.fold_in(key_of[4], part), 71), part)
    lengths = uneven_parts(part_keys[1], R, TOTAL_PAGES, MOST, 2).astype(jnp.int32)
    k_cache = draw_k_cache(jax.random.fold_in(jax.random.fold_in(key_of[4], part), 71), part)
    v_cache = centred(part_keys[3], (TOKENS, KVH, HD), 1.0, 6.0, ((0, 8), (1, 2)))
    return {"queries": queries, "lengths": lengths, "k_cache": k_cache, "v_cache": v_cache}


lowest_score = -1e30


def reference(queries, lengths, k_cache, v_cache):
    request_count = queries.shape[0]
    query_heads = queries.shape[1]
    head_width = queries.shape[2]
    key_heads = k_cache.shape[1]
    group_size = query_heads // key_heads
    page_count = k_cache.shape[0] // PAGE
    scale = float(head_width) ** -0.5
    starts = (jnp.cumsum(lengths) - lengths).astype(jnp.int32)
    page_ids = jnp.arange(page_count, dtype=jnp.int32)
    owner = (jnp.sum((starts[None, :] <= page_ids[:, None]).astype(jnp.int32), axis=1) - 1).astype(jnp.int32)
    page_query = jnp.take(queries, owner, axis=0).reshape(page_count, key_heads, group_size, head_width)
    key_pages = k_cache.reshape(page_count, PAGE, key_heads, head_width)
    value_pages = v_cache.reshape(page_count, PAGE, key_heads, head_width)
    block = math.gcd(64, page_count)
    blocks = page_count // block

    def one_block(pieces):
        query_block, key_block, value_block = pieces
        scores = jnp.einsum("pskd,pkgd->pkgs", key_block.astype(jnp.float32), query_block.astype(jnp.float32)) * scale
        page_max = jnp.max(scores, axis=3)
        weights = jnp.exp(scores - page_max[..., None])
        page_sum = jnp.sum(weights, axis=3)
        rounded = lax.optimization_barrier(weights.astype(jnp.bfloat16)).astype(jnp.float32)
        page_out = jnp.einsum("pkgs,pskd->pkgd", rounded, value_block.astype(jnp.float32))
        return page_max, page_sum, page_out

    page_max, page_sum, page_out = lax.map(one_block, (
        page_query.reshape(blocks, block, key_heads, group_size, head_width),
        key_pages.reshape(blocks, block, PAGE, key_heads, head_width),
        value_pages.reshape(blocks, block, PAGE, key_heads, head_width)))
    page_max = page_max.reshape(page_count, key_heads, group_size)
    page_sum = page_sum.reshape(page_count, key_heads, group_size)
    page_out = page_out.reshape(page_count, key_heads, group_size, head_width)
    member = owner[:, None] == jnp.arange(request_count, dtype=jnp.int32)[None, :]
    request_max = jnp.max(jnp.where(member[:, :, None, None], page_max[:, None], lowest_score), axis=0)
    rescale = jnp.exp(page_max - jnp.take(request_max, owner, axis=0))
    numer = jax.ops.segment_sum(rescale[..., None] * page_out, owner, num_segments=request_count)
    denom = jax.ops.segment_sum(rescale * page_sum, owner, num_segments=request_count)
    attended = numer / denom[..., None]
    return attended.reshape(request_count, query_heads, head_width).astype(jnp.bfloat16)
```

```python
import functools
import math

import jax
import jax.numpy as jnp
from jax import lax
from jax.experimental import pallas as pl
from jax.experimental.pallas import tpu as pltpu
from jax.sharding import PartitionSpec as P

PAGE = 128
MESH = pl.DeviceIdType.MESH
LOWEST = -1e30


def kernel(
    n, subs, pages, unroll, key_heads, own_requests, group_size, head_width,
    q_in, len_in, k_in, v_in, out_ref,
    q_all, len_all, k_buf, v_buf, s_buf, m_buf, send, recv,
    q_sems, len_sems, k_sems, v_sems, send_sems, recv_sems,
):
    requests = own_requests * subs
    query_heads = key_heads * group_size
    own_heads = query_heads // subs
    rows = PAGE * key_heads
    steps = pages // unroll
    span = rows * unroll
    sub = lax.axis_index("sub")
    me = lax.axis_index("seq") * subs + sub

    def k_copy(i):
        at = pl.ds(pl.multiple_of(i * span, span), span)
        return pltpu.make_async_copy(k_in.at[at], k_buf.at[at], k_sems.at[i])

    def v_copy(i):
        at = pl.ds(pl.multiple_of(i * span, span), span)
        return pltpu.make_async_copy(v_in.at[at], v_buf.at[at], v_sems.at[i])

    def peer(k):
        other = lax.rem(me + k, n)
        return other // subs, lax.rem(other, subs)

    barrier = pltpu.get_barrier_semaphore()
    for k in range(1, n):
        other_seq, other_sub = peer(k)
        pl.semaphore_signal(
            barrier, inc=1, device_id={"seq": other_seq, "sub": other_sub}, device_id_type=MESH
        )
    own_q = pltpu.make_async_copy(q_in, q_all.at[sub], q_sems.at[0])
    own_q.start()
    own_len = pltpu.make_async_copy(len_in, len_all.at[sub], len_sems.at[0])
    own_len.start()
    for i in range(steps):
        k_copy(i).start()
    for i in range(steps):
        v_copy(i).start()
    pl.semaphore_wait(barrier, n - 1)

    copies = []
    for k in range(1, subs):
        other = {"sub": lax.rem(sub + k, subs)}
        copies.append(pltpu.make_async_remote_copy(
            src_ref=q_all.at[sub], dst_ref=q_all.at[sub], send_sem=q_sems.at[2 * k - 1],
            recv_sem=q_sems.at[2 * k], device_id=other, device_id_type=MESH,
        ))
        copies.append(pltpu.make_async_remote_copy(
            src_ref=len_all.at[sub], dst_ref=len_all.at[sub], send_sem=len_sems.at[2 * k - 1],
            recv_sem=len_sems.at[2 * k], device_id=other, device_id_type=MESH,
        ))
    own_q.wait()
    own_len.wait()
    for copy in copies:
        copy.start()
    for copy in copies:
        copy.wait()

    starts, total = [], jnp.int32(0)
    for r in range(requests):
        starts.append(total)
        total = total + len_all[r // own_requests, 0, r % own_requests]
    first_page = me * pages

    def owner_of(page):
        owner = jnp.int32(-1)
        for start in starts:
            owner = owner + (start <= first_page + page).astype(jnp.int32)
        return owner

    lane = lax.broadcasted_iota(jnp.int32, (query_heads, rows), 1)
    row = lax.broadcasted_iota(jnp.int32, (query_heads, rows), 0)
    matching = lax.rem(lane, key_heads) == row // group_size
    contract_last = (((1,), (1,)), ((), ()))

    def scores(i, highest):
        k_copy(i).wait()
        for j in range(unroll):
            page = i * unroll + j
            owner = owner_of(page)
            query = q_all[owner // own_requests, lax.rem(owner, own_requests)]
            at = pl.ds(pl.multiple_of(page * rows, rows), rows)
            score = lax.dot_general(
                query, k_buf[at, :], contract_last, preferred_element_type=jnp.float32
            )
            score = jnp.where(matching, score, LOWEST)
            s_buf[page] = score
            top = score[:, :head_width]
            for c in range(1, rows // head_width):
                top = jnp.maximum(top, score[:, c * head_width:(c + 1) * head_width])
            highest = tuple(
                jnp.maximum(highest[r], jnp.where(owner == r, top, LOWEST)) for r in range(requests)
            )
        return highest

    lowest = jnp.full((query_heads, head_width), LOWEST, jnp.float32)
    highest = lax.fori_loop(0, steps, scores, (lowest,) * requests)
    local_max = []
    for r in range(requests):
        top = jnp.broadcast_to(jnp.max(highest[r], axis=1, keepdims=True), lowest.shape)
        m_buf[r] = top
        local_max.append(top)

    factor = float(head_width) ** -0.5 * math.log2(math.e)
    repeat = rows // head_width

    def values(i, so_far):
        v_copy(i).wait()
        sums, outs = so_far
        for j in range(unroll):
            page = i * unroll + j
            owner = owner_of(page)
            top = m_buf[owner]
            at = pl.ds(pl.multiple_of(page * rows, rows), rows)
            pieces = [
                jnp.exp2((s_buf[page, :, c * head_width:(c + 1) * head_width] - top) * factor)
                for c in range(repeat)
            ]
            page_sum = pieces[0]
            for piece in pieces[1:]:
                page_sum = page_sum + piece
            weights = jnp.concatenate([piece.astype(jnp.bfloat16) for piece in pieces], axis=1)
            page_out = jnp.dot(weights, v_buf[at, :], preferred_element_type=jnp.float32)
            sums = tuple(sums[r] + jnp.where(owner == r, page_sum, 0.0) for r in range(requests))
            outs = tuple(outs[r] + jnp.where(owner == r, page_out, 0.0) for r in range(requests))
        return sums, outs

    zero = jnp.zeros((query_heads, head_width), jnp.float32)
    sums, outs = lax.fori_loop(0, steps, values, ((zero,) * requests, (zero,) * requests))

    low_lanes = lax.broadcasted_iota(jnp.int32, zero.shape, 1) < head_width // 2
    for r in range(requests):
        local_sum = jnp.broadcast_to(jnp.sum(sums[r], axis=1, keepdims=True), zero.shape)
        stats = jnp.where(low_lanes, local_max[r], local_sum)
        for half in range(subs):
            part = slice(half * own_heads, (half + 1) * own_heads)
            send[half, r] = outs[r][part]
            send[half, requests + r] = stats[part]

    copies = []
    for k in range(1, n):
        other_seq, other_sub = peer(k)
        copies.append(pltpu.make_async_remote_copy(
            src_ref=send.at[other_sub], dst_ref=recv.at[k - 1], send_sem=send_sems.at[k - 1],
            recv_sem=recv_sems.at[k - 1], device_id={"seq": other_seq, "sub": other_sub},
            device_id_type=MESH,
        ))
        copies[-1].start()
    for copy in copies:
        copy.wait_recv()

    half_width = head_width // 2
    for r in range(requests):
        parts = [(send[sub, requests + r], send[sub, r])]
        for k in range(n - 1):
            parts.append((recv[k, requests + r], recv[k, r]))
        top = parts[0][0]
        for stats, _ in parts[1:]:
            top = jnp.maximum(top, stats)
        top = top[:, :1]
        denominator = jnp.zeros((own_heads, 1), jnp.float32)
        numerator = jnp.zeros((own_heads, head_width), jnp.float32)
        for stats, out in parts:
            lift = jnp.exp2((stats[:, :1] - top) * factor)
            denominator = denominator + lift * stats[:, half_width:half_width + 1]
            numerator = numerator + lift * out
        out_ref[r] = (numerator / denominator).astype(out_ref.dtype)
    for copy in copies:
        copy.wait_send()


def shards(seqs, subs, queries, lengths, k_cache, v_cache):
    tokens, key_heads, head_width = k_cache.shape
    own_requests, query_heads, _ = queries.shape
    group_size = query_heads // key_heads
    requests = own_requests * subs
    pages = tokens // PAGE
    unroll = math.gcd(4, pages)
    steps = pages // unroll
    rows = PAGE * key_heads
    n = seqs * subs
    own_heads = query_heads // subs
    anywhere = pl.BlockSpec(memory_space=pltpu.HBM)
    sems = pltpu.SemaphoreType.DMA
    return pl.pallas_call(
        functools.partial(
            kernel, n, subs, pages, unroll, key_heads, own_requests, group_size, head_width
        ),
        out_shape=jax.ShapeDtypeStruct((requests, own_heads, head_width), jnp.bfloat16),
        in_specs=[anywhere] * 4,
        out_specs=pl.BlockSpec(memory_space=pltpu.VMEM),
        scratch_shapes=[
            pltpu.VMEM((subs, own_requests, query_heads, head_width), jnp.bfloat16),
            pltpu.SMEM((subs, 1, own_requests), jnp.int32),
            pltpu.VMEM((tokens * key_heads, head_width), jnp.bfloat16),
            pltpu.VMEM((tokens * key_heads, head_width), jnp.bfloat16),
            pltpu.VMEM((pages, query_heads, rows), jnp.float32),
            pltpu.VMEM((requests, query_heads, head_width), jnp.float32),
            pltpu.VMEM((subs, 2 * requests, own_heads, head_width), jnp.float32),
            pltpu.VMEM((n - 1, 2 * requests, own_heads, head_width), jnp.float32),
            sems((2 * subs - 1,)),
            sems((2 * subs - 1,)),
            sems((steps,)),
            sems((steps,)),
            sems((n - 1,)),
            sems((n - 1,)),
        ],
        compiler_params=pltpu.CompilerParams(
            collective_id=0, has_side_effects=True, vmem_limit_bytes=63 * 1024 * 1024
        ),
    )(
        queries,
        lengths.reshape(1, own_requests),
        k_cache.reshape(tokens * key_heads, head_width),
        v_cache.reshape(tokens * key_heads, head_width),
    )


def solution(mesh):
    return jax.shard_map(
        functools.partial(shards, mesh.shape["seq"], mesh.shape["sub"]),
        mesh=mesh,
        in_specs=(
            P(("group", "sub"), "head", None),
            P(("group", "sub")),
            P(("group", "seq", "sub"), "head", None),
            P(("group", "seq", "sub"), "head", None),
        ),
        out_specs=P("group", ("head", "sub"), None),
        check_vma=False,
    )
```

```python
import functools
import math

import jax
import jax.numpy as jnp
from jax import lax
from jax.experimental import pallas as pl
from jax.experimental.pallas import tpu as pltpu
from jax.sharding import PartitionSpec as P

PAGE = 128
MESH = pl.DeviceIdType.MESH
LOWEST = -1e30


def kernel(
    n, subs, pages, unroll, key_heads, own_requests, group_size, head_width,
    q_in, len_in, k_in, v_in, out_ref,
    q_all, len_all, k_buf, v_buf, s_buf, m_buf, send, recv,
    q_sems, len_sems, k_sems, v_sems, send_sems, recv_sems,
):
    requests = own_requests * subs
    query_heads = key_heads * group_size
    own_heads = query_heads // subs
    rows = PAGE * key_heads
    steps = pages // unroll
    span = rows * unroll
    sub = lax.axis_index("sub")
    me = lax.axis_index("seq") * subs + sub

    def k_copy(i):
        at = pl.ds(pl.multiple_of(i * span, span), span)
        return pltpu.make_async_copy(k_in.at[at], k_buf.at[at], k_sems.at[i])

    def v_copy(i):
        at = pl.ds(pl.multiple_of(i * span, span), span)
        return pltpu.make_async_copy(v_in.at[at], v_buf.at[at], v_sems.at[i])

    def peer(k):
        other = lax.rem(me + k, n)
        return other // subs, lax.rem(other, subs)

    barrier = pltpu.get_barrier_semaphore()
    for k in range(1, n):
        other_seq, other_sub = peer(k)
        pl.semaphore_signal(
            barrier, inc=1, device_id={"seq": other_seq, "sub": other_sub}, device_id_type=MESH
        )
    own_q = pltpu.make_async_copy(q_in, q_all.at[sub], q_sems.at[0])
    own_q.start()
    own_len = pltpu.make_async_copy(len_in, len_all.at[sub], len_sems.at[0])
    own_len.start()
    for i in range(steps):
        k_copy(i).start()
        v_copy(i).start()
    pl.semaphore_wait(barrier, n - 1)

    copies = []
    for k in range(1, subs):
        other = {"sub": lax.rem(sub + k, subs)}
        copies.append(pltpu.make_async_remote_copy(
            src_ref=q_all.at[sub], dst_ref=q_all.at[sub], send_sem=q_sems.at[2 * k - 1],
            recv_sem=q_sems.at[2 * k], device_id=other, device_id_type=MESH,
        ))
        copies.append(pltpu.make_async_remote_copy(
            src_ref=len_all.at[sub], dst_ref=len_all.at[sub], send_sem=len_sems.at[2 * k - 1],
            recv_sem=len_sems.at[2 * k], device_id=other, device_id_type=MESH,
        ))
    own_q.wait()
    own_len.wait()
    for copy in copies:
        copy.start()
    for copy in copies:
        copy.wait()

    starts, total = [], jnp.int32(0)
    for r in range(requests):
        starts.append(total)
        total = total + len_all[r // own_requests, 0, r % own_requests]
    first_page = me * pages

    def owner_of(page):
        owner = jnp.int32(-1)
        for start in starts:
            owner = owner + (start <= first_page + page).astype(jnp.int32)
        return owner

    lane = lax.broadcasted_iota(jnp.int32, (query_heads, rows), 1)
    row = lax.broadcasted_iota(jnp.int32, (query_heads, rows), 0)
    matching = lax.rem(lane, key_heads) == row // group_size
    contract_last = (((1,), (1,)), ((), ()))

    factor = float(head_width) ** -0.5 * math.log2(math.e)
    repeat = rows // head_width
    lowest = jnp.full((query_heads, head_width), LOWEST, jnp.float32)

    def attend(i, highest):
        k_copy(i).wait()
        owners, all_scores = [], []
        for j in range(unroll):
            page = i * unroll + j
            owner = owner_of(page)
            owners.append(owner)
            query = q_all[owner // own_requests, lax.rem(owner, own_requests)]
            at = pl.ds(pl.multiple_of(page * rows, rows), rows)
            score = lax.dot_general(
                query, k_buf[at, :], contract_last, preferred_element_type=jnp.float32
            )
            all_scores.append(jnp.where(matching, score, LOWEST))
        v_copy(i).wait()
        for j in range(unroll):
            page, owner, score = i * unroll + j, owners[j], all_scores[j]
            top = score[:, :head_width]
            for c in range(1, repeat):
                top = jnp.maximum(top, score[:, c * head_width:(c + 1) * head_width])
            top = jnp.broadcast_to(jnp.max(top, axis=1, keepdims=True), lowest.shape)
            pieces = [
                jnp.exp2((score[:, c * head_width:(c + 1) * head_width] - top) * factor)
                for c in range(repeat)
            ]
            page_sum = pieces[0]
            for piece in pieces[1:]:
                page_sum = page_sum + piece
            weights = jnp.concatenate([piece.astype(jnp.bfloat16) for piece in pieces], axis=1)
            at = pl.ds(pl.multiple_of(page * rows, rows), rows)
            s_buf[page, 0] = top
            s_buf[page, 1] = page_sum
            s_buf[page, 2] = jnp.dot(weights, v_buf[at, :], preferred_element_type=jnp.float32)
            highest = tuple(
                jnp.maximum(highest[r], jnp.where(owner == r, top, LOWEST)) for r in range(requests)
            )
        return highest

    local_max = lax.fori_loop(0, steps, attend, (lowest,) * requests)
    for r in range(requests):
        m_buf[r] = local_max[r]

    def combine(i, so_far):
        sums, outs = so_far
        for j in range(unroll):
            page = i * unroll + j
            owner = owner_of(page)
            lift = jnp.exp2((s_buf[page, 0] - m_buf[owner]) * factor)
            page_sum = lift * s_buf[page, 1]
            page_out = lift * s_buf[page, 2]
            sums = tuple(sums[r] + jnp.where(owner == r, page_sum, 0.0) for r in range(requests))
            outs = tuple(outs[r] + jnp.where(owner == r, page_out, 0.0) for r in range(requests))
        return sums, outs

    zero = jnp.zeros((query_heads, head_width), jnp.float32)
    sums, outs = lax.fori_loop(0, steps, combine, ((zero,) * requests, (zero,) * requests))

    low_lanes = lax.broadcasted_iota(jnp.int32, zero.shape, 1) < head_width // 2
    for r in range(requests):
        local_sum = jnp.broadcast_to(jnp.sum(sums[r], axis=1, keepdims=True), zero.shape)
        stats = jnp.where(low_lanes, local_max[r], local_sum)
        for half in range(subs):
            part = slice(half * own_heads, (half + 1) * own_heads)
            send[half, r] = outs[r][part]
            send[half, requests + r] = stats[part]

    copies = []
    for k in range(1, n):
        other_seq, other_sub = peer(k)
        copies.append(pltpu.make_async_remote_copy(
            src_ref=send.at[other_sub], dst_ref=recv.at[k - 1], send_sem=send_sems.at[k - 1],
            recv_sem=recv_sems.at[k - 1], device_id={"seq": other_seq, "sub": other_sub},
            device_id_type=MESH,
        ))
        copies[-1].start()
    for copy in copies:
        copy.wait_recv()

    half_width = head_width // 2
    for r in range(requests):
        parts = [(send[sub, requests + r], send[sub, r])]
        for k in range(n - 1):
            parts.append((recv[k, requests + r], recv[k, r]))
        top = parts[0][0]
        for stats, _ in parts[1:]:
            top = jnp.maximum(top, stats)
        top = top[:, :1]
        denominator = jnp.zeros((own_heads, 1), jnp.float32)
        numerator = jnp.zeros((own_heads, head_width), jnp.float32)
        for stats, out in parts:
            lift = jnp.exp2((stats[:, :1] - top) * factor)
            denominator = denominator + lift * stats[:, half_width:half_width + 1]
            numerator = numerator + lift * out
        out_ref[r] = (numerator / denominator).astype(out_ref.dtype)
    for copy in copies:
        copy.wait_send()


def shards(seqs, subs, queries, lengths, k_cache, v_cache):
    tokens, key_heads, head_width = k_cache.shape
    own_requests, query_heads, _ = queries.shape
    group_size = query_heads // key_heads
    requests = own_requests * subs
    pages = tokens // PAGE
    unroll = math.gcd(8, pages)
    steps = pages // unroll
    rows = PAGE * key_heads
    n = seqs * subs
    own_heads = query_heads // subs
    anywhere = pl.BlockSpec(memory_space=pltpu.HBM)
    sems = pltpu.SemaphoreType.DMA
    return pl.pallas_call(
        functools.partial(
            kernel, n, subs, pages, unroll, key_heads, own_requests, group_size, head_width
        ),
        out_shape=jax.ShapeDtypeStruct((requests, own_heads, head_width), jnp.bfloat16),
        in_specs=[anywhere] * 4,
        out_specs=pl.BlockSpec(memory_space=pltpu.VMEM),
        scratch_shapes=[
            pltpu.VMEM((subs, own_requests, query_heads, head_width), jnp.bfloat16),
            pltpu.SMEM((subs, 1, own_requests), jnp.int32),
            pltpu.VMEM((tokens * key_heads, head_width), jnp.bfloat16),
            pltpu.VMEM((tokens * key_heads, head_width), jnp.bfloat16),
            pltpu.VMEM((pages, 3, query_heads, head_width), jnp.float32),
            pltpu.VMEM((requests, query_heads, head_width), jnp.float32),
            pltpu.VMEM((subs, 2 * requests, own_heads, head_width), jnp.float32),
            pltpu.VMEM((n - 1, 2 * requests, own_heads, head_width), jnp.float32),
            sems((2 * subs - 1,)),
            sems((2 * subs - 1,)),
            sems((steps,)),
            sems((steps,)),
            sems((n - 1,)),
            sems((n - 1,)),
        ],
        compiler_params=pltpu.CompilerParams(
            collective_id=0, has_side_effects=True, vmem_limit_bytes=63 * 1024 * 1024
        ),
    )(
        queries,
        lengths.reshape(1, own_requests),
        k_cache.reshape(tokens * key_heads, head_width),
        v_cache.reshape(tokens * key_heads, head_width),
    )


def solution(mesh):
    return jax.shard_map(
        functools.partial(shards, mesh.shape["seq"], mesh.shape["sub"]),
        mesh=mesh,
        in_specs=(
            P(("group", "sub"), "head", None),
            P(("group", "sub")),
            P(("group", "seq", "sub"), "head", None),
            P(("group", "seq", "sub"), "head", None),
        ),
        out_specs=P("group", ("head", "sub"), None),
        check_vma=False,
    )
```

```python
import functools
import math

import jax
import jax.numpy as jnp
from jax import lax
from jax.experimental import pallas as pl
from jax.experimental.pallas import tpu as pltpu
from jax.sharding import PartitionSpec as P

PAGE = 128
MESH = pl.DeviceIdType.MESH
LOWEST = -1e30


def kernel(
    n, subs, pages, unroll, key_heads, own_requests, group_size, head_width,
    q_in, len_in, k_in, v_in, out_ref,
    q_all, len_all, k_buf, v_buf, s_buf, m_buf, send, recv, send_stats, recv_stats,
    q_sems, len_sems, k_sems, v_sems, send_sems, recv_sems,
    stat_send_sems, stat_recv_sems,
):
    requests = own_requests * subs
    query_heads = key_heads * group_size
    own_heads = query_heads // subs
    rows = PAGE * key_heads
    steps = pages // unroll
    span = rows * unroll
    sub = lax.axis_index("sub")
    me = lax.axis_index("seq") * subs + sub

    def k_copy(i):
        at = pl.ds(pl.multiple_of(i * span, span), span)
        return pltpu.make_async_copy(k_in.at[at], k_buf.at[at], k_sems.at[i])

    def v_copy(i):
        at = pl.ds(pl.multiple_of(i * span, span), span)
        return pltpu.make_async_copy(v_in.at[at], v_buf.at[at], v_sems.at[i])

    def peer(k):
        other = lax.rem(me + k, n)
        return other // subs, lax.rem(other, subs)

    barrier = pltpu.get_barrier_semaphore()
    for k in range(1, n):
        other_seq, other_sub = peer(k)
        pl.semaphore_signal(
            barrier, inc=1, device_id={"seq": other_seq, "sub": other_sub}, device_id_type=MESH
        )
    own_q = pltpu.make_async_copy(q_in, q_all.at[sub], q_sems.at[0])
    own_q.start()
    own_len = pltpu.make_async_copy(len_in, len_all.at[sub], len_sems.at[0])
    own_len.start()
    for i in range(steps):
        k_copy(i).start()
        v_copy(i).start()
    pl.semaphore_wait(barrier, n - 1)

    copies = []
    for k in range(1, subs):
        other = {"sub": lax.rem(sub + k, subs)}
        copies.append(pltpu.make_async_remote_copy(
            src_ref=q_all.at[sub], dst_ref=q_all.at[sub], send_sem=q_sems.at[2 * k - 1],
            recv_sem=q_sems.at[2 * k], device_id=other, device_id_type=MESH,
        ))
        copies.append(pltpu.make_async_remote_copy(
            src_ref=len_all.at[sub], dst_ref=len_all.at[sub], send_sem=len_sems.at[2 * k - 1],
            recv_sem=len_sems.at[2 * k], device_id=other, device_id_type=MESH,
        ))
    own_q.wait()
    own_len.wait()
    for copy in copies:
        copy.start()
    for copy in copies:
        copy.wait()

    starts, total = [], jnp.int32(0)
    for r in range(requests):
        starts.append(total)
        total = total + len_all[r // own_requests, 0, r % own_requests]
    first_page = me * pages

    def owner_of(page):
        owner = jnp.int32(-1)
        for start in starts:
            owner = owner + (start <= first_page + page).astype(jnp.int32)
        return owner

    lane = lax.broadcasted_iota(jnp.int32, (query_heads, rows), 1)
    row = lax.broadcasted_iota(jnp.int32, (query_heads, rows), 0)
    matching = lax.rem(lane, key_heads) == row // group_size
    contract_last = (((1,), (1,)), ((), ()))

    factor = float(head_width) ** -0.5 * math.log2(math.e)
    repeat = rows // head_width
    lowest = jnp.full((query_heads, head_width), LOWEST, jnp.float32)

    def attend(i, highest):
        k_copy(i).wait()
        owners, all_scores = [], []
        for j in range(unroll):
            page = i * unroll + j
            owner = owner_of(page)
            owners.append(owner)
            query = q_all[owner // own_requests, lax.rem(owner, own_requests)]
            at = pl.ds(pl.multiple_of(page * rows, rows), rows)
            score = lax.dot_general(
                query, k_buf[at, :], contract_last, preferred_element_type=jnp.float32
            )
            all_scores.append(jnp.where(matching, score, LOWEST))
        v_copy(i).wait()
        for j in range(unroll):
            page, owner, score = i * unroll + j, owners[j], all_scores[j]
            top = score[:, :head_width]
            for c in range(1, repeat):
                top = jnp.maximum(top, score[:, c * head_width:(c + 1) * head_width])
            top = jnp.broadcast_to(jnp.max(top, axis=1, keepdims=True), lowest.shape)
            pieces = [
                jnp.exp2((score[:, c * head_width:(c + 1) * head_width] - top) * factor)
                for c in range(repeat)
            ]
            page_sum = pieces[0]
            for piece in pieces[1:]:
                page_sum = page_sum + piece
            weights = jnp.concatenate([piece.astype(jnp.bfloat16) for piece in pieces], axis=1)
            at = pl.ds(pl.multiple_of(page * rows, rows), rows)
            s_buf[page, 0] = top
            s_buf[page, 1] = page_sum
            s_buf[page, 2] = jnp.dot(weights, v_buf[at, :], preferred_element_type=jnp.float32)
            highest = tuple(
                jnp.maximum(highest[r], jnp.where(owner == r, top, LOWEST)) for r in range(requests)
            )
        return highest

    local_max = lax.fori_loop(0, steps, attend, (lowest,) * requests)
    for r in range(requests):
        m_buf[r] = local_max[r]

    def combine(i, so_far):
        sums, outs = so_far
        for j in range(unroll):
            page = i * unroll + j
            owner = owner_of(page)
            lift = jnp.exp2((s_buf[page, 0] - m_buf[owner]) * factor)
            page_sum = lift * s_buf[page, 1]
            page_out = lift * s_buf[page, 2]
            sums = tuple(sums[r] + jnp.where(owner == r, page_sum, 0.0) for r in range(requests))
            outs = tuple(outs[r] + jnp.where(owner == r, page_out, 0.0) for r in range(requests))
        return sums, outs

    zero = jnp.zeros((query_heads, head_width), jnp.float32)
    sums, outs = lax.fori_loop(0, steps, combine, ((zero,) * requests, (zero,) * requests))

    stat_lane = lax.broadcasted_iota(jnp.int32, zero.shape, 1)
    stats = zero
    for r in range(requests):
        local_sum = jnp.broadcast_to(jnp.sum(sums[r], axis=1, keepdims=True), zero.shape)
        stats = jnp.where(stat_lane == 2 * r, local_max[r], stats)
        stats = jnp.where(stat_lane == 2 * r + 1, local_sum, stats)
    for half in range(subs):
        part = slice(half * own_heads, (half + 1) * own_heads)
        send_stats[half] = stats[part]
        for r in range(requests):
            send[half, r] = outs[r][part].astype(jnp.bfloat16)

    copies = []
    for k in range(1, n):
        other_seq, other_sub = peer(k)
        other = {"seq": other_seq, "sub": other_sub}
        copies.append(pltpu.make_async_remote_copy(
            src_ref=send_stats.at[other_sub], dst_ref=recv_stats.at[k - 1],
            send_sem=stat_send_sems.at[k - 1], recv_sem=stat_recv_sems.at[k - 1],
            device_id=other, device_id_type=MESH,
        ))
        copies[-1].start()
        copies.append(pltpu.make_async_remote_copy(
            src_ref=send.at[other_sub], dst_ref=recv.at[k - 1], send_sem=send_sems.at[k - 1],
            recv_sem=recv_sems.at[k - 1], device_id=other, device_id_type=MESH,
        ))
        copies[-1].start()
    for copy in copies:
        copy.wait_recv()

    all_stats = [send_stats[sub]] + [recv_stats[k] for k in range(n - 1)]
    top = all_stats[0]
    for part in all_stats[1:]:
        top = jnp.maximum(top, part)
    for r in range(requests):
        denominator = jnp.zeros((own_heads, 1), jnp.float32)
        numerator = jnp.zeros((own_heads, head_width), jnp.float32)
        for k, part in enumerate(all_stats):
            out = send[sub, r] if k == 0 else recv[k - 1, r]
            lift = jnp.exp2((part[:, 2 * r:2 * r + 1] - top[:, 2 * r:2 * r + 1]) * factor)
            denominator = denominator + lift * part[:, 2 * r + 1:2 * r + 2]
            numerator = numerator + lift * out.astype(jnp.float32)
        out_ref[r] = (numerator / denominator).astype(out_ref.dtype)
    for copy in copies:
        copy.wait_send()


def shards(seqs, subs, queries, lengths, k_cache, v_cache):
    tokens, key_heads, head_width = k_cache.shape
    own_requests, query_heads, _ = queries.shape
    group_size = query_heads // key_heads
    requests = own_requests * subs
    pages = tokens // PAGE
    unroll = math.gcd(8, pages)
    steps = pages // unroll
    rows = PAGE * key_heads
    n = seqs * subs
    own_heads = query_heads // subs
    anywhere = pl.BlockSpec(memory_space=pltpu.HBM)
    sems = pltpu.SemaphoreType.DMA
    return pl.pallas_call(
        functools.partial(
            kernel, n, subs, pages, unroll, key_heads, own_requests, group_size, head_width
        ),
        out_shape=jax.ShapeDtypeStruct((requests, own_heads, head_width), jnp.bfloat16),
        in_specs=[anywhere] * 4,
        out_specs=pl.BlockSpec(memory_space=pltpu.VMEM),
        scratch_shapes=[
            pltpu.VMEM((subs, own_requests, query_heads, head_width), jnp.bfloat16),
            pltpu.SMEM((subs, 1, own_requests), jnp.int32),
            pltpu.VMEM((tokens * key_heads, head_width), jnp.bfloat16),
            pltpu.VMEM((tokens * key_heads, head_width), jnp.bfloat16),
            pltpu.VMEM((pages, 3, query_heads, head_width), jnp.float32),
            pltpu.VMEM((requests, query_heads, head_width), jnp.float32),
            pltpu.VMEM((subs, requests, own_heads, head_width), jnp.bfloat16),
            pltpu.VMEM((n - 1, requests, own_heads, head_width), jnp.bfloat16),
            pltpu.VMEM((subs, own_heads, head_width), jnp.float32),
            pltpu.VMEM((n - 1, own_heads, head_width), jnp.float32),
            sems((2 * subs - 1,)),
            sems((2 * subs - 1,)),
            sems((steps,)),
            sems((steps,)),
            sems((n - 1,)),
            sems((n - 1,)),
            sems((n - 1,)),
            sems((n - 1,)),
        ],
        compiler_params=pltpu.CompilerParams(
            collective_id=0, has_side_effects=True, vmem_limit_bytes=63 * 1024 * 1024
        ),
    )(
        queries,
        lengths.reshape(1, own_requests),
        k_cache.reshape(tokens * key_heads, head_width),
        v_cache.reshape(tokens * key_heads, head_width),
    )


def solution(mesh):
    return jax.shard_map(
        functools.partial(shards, mesh.shape["seq"], mesh.shape["sub"]),
        mesh=mesh,
        in_specs=(
            P(("group", "sub"), "head", None),
            P(("group", "sub")),
            P(("group", "seq", "sub"), "head", None),
            P(("group", "seq", "sub"), "head", None),
        ),
        out_specs=P("group", ("head", "sub"), None),
        check_vma=False,
    )
```

```python
import functools
import math

import jax
import jax.numpy as jnp
from jax import lax
from jax.experimental import pallas as pl
from jax.experimental.pallas import tpu as pltpu
from jax.sharding import PartitionSpec as P

PAGE = 128
MESH = pl.DeviceIdType.MESH
LOWEST = -1e30


def kernel(
    n, subs, pages, unroll, key_heads, own_requests, group_size, head_width,
    q_in, len_in, k_in, v_in, out_ref,
    q_all, len_all, k_buf, v_buf, s_buf, m_buf, send, recv,
    q_sems, len_sems, k_sems, v_sems, send_sems, recv_sems,
):
    requests = own_requests * subs
    query_heads = key_heads * group_size
    own_heads = query_heads // subs
    rows = PAGE * key_heads
    steps = pages // unroll
    span = rows * unroll
    sub = lax.axis_index("sub")
    me = lax.axis_index("seq") * subs + sub

    def k_copy(i):
        at = pl.ds(pl.multiple_of(i * span, span), span)
        return pltpu.make_async_copy(k_in.at[at], k_buf.at[at], k_sems.at[i])

    def v_copy(i):
        at = pl.ds(pl.multiple_of(i * span, span), span)
        return pltpu.make_async_copy(v_in.at[at], v_buf.at[at], v_sems.at[i])

    def peer(k):
        other = lax.rem(me + k, n)
        return other // subs, lax.rem(other, subs)

    barrier = pltpu.get_barrier_semaphore()
    for k in range(1, n):
        other_seq, other_sub = peer(k)
        pl.semaphore_signal(
            barrier, inc=1, device_id={"seq": other_seq, "sub": other_sub}, device_id_type=MESH
        )
    own_q = pltpu.make_async_copy(q_in, q_all.at[sub], q_sems.at[0])
    own_q.start()
    own_len = pltpu.make_async_copy(len_in, len_all.at[sub], len_sems.at[0])
    own_len.start()
    for i in range(steps):
        k_copy(i).start()
        v_copy(i).start()
    pl.semaphore_wait(barrier, n - 1)

    copies = []
    for k in range(1, subs):
        other = {"sub": lax.rem(sub + k, subs)}
        copies.append(pltpu.make_async_remote_copy(
            src_ref=q_all.at[sub], dst_ref=q_all.at[sub], send_sem=q_sems.at[2 * k - 1],
            recv_sem=q_sems.at[2 * k], device_id=other, device_id_type=MESH,
        ))
        copies.append(pltpu.make_async_remote_copy(
            src_ref=len_all.at[sub], dst_ref=len_all.at[sub], send_sem=len_sems.at[2 * k - 1],
            recv_sem=len_sems.at[2 * k], device_id=other, device_id_type=MESH,
        ))
    own_q.wait()
    own_len.wait()
    for copy in copies:
        copy.start()
    for copy in copies:
        copy.wait()

    starts, total = [], jnp.int32(0)
    for r in range(requests):
        starts.append(total)
        total = total + len_all[r // own_requests, 0, r % own_requests]
    first_page = me * pages

    def owner_of(page):
        owner = jnp.int32(-1)
        for start in starts:
            owner = owner + (start <= first_page + page).astype(jnp.int32)
        return owner

    lane = lax.broadcasted_iota(jnp.int32, (query_heads, rows), 1)
    row = lax.broadcasted_iota(jnp.int32, (query_heads, rows), 0)
    matching = lax.rem(lane, key_heads) == row // group_size
    contract_last = (((1,), (1,)), ((), ()))

    factor = float(head_width) ** -0.5 * math.log2(math.e)
    repeat = rows // head_width
    lowest = jnp.full((query_heads, head_width), LOWEST, jnp.float32)

    def attend(i, highest):
        k_copy(i).wait()
        owners, all_scores = [], []
        for j in range(unroll):
            page = i * unroll + j
            owner = owner_of(page)
            owners.append(owner)
            query = q_all[owner // own_requests, lax.rem(owner, own_requests)]
            at = pl.ds(pl.multiple_of(page * rows, rows), rows)
            score = lax.dot_general(
                query, k_buf[at, :], contract_last, preferred_element_type=jnp.float32
            )
            all_scores.append(jnp.where(matching, score, LOWEST))
        v_copy(i).wait()
        for j in range(unroll):
            page, owner, score = i * unroll + j, owners[j], all_scores[j]
            top = score[:, :head_width]
            for c in range(1, repeat):
                top = jnp.maximum(top, score[:, c * head_width:(c + 1) * head_width])
            top = jnp.broadcast_to(jnp.max(top, axis=1, keepdims=True), lowest.shape)
            pieces = [
                jnp.exp2((score[:, c * head_width:(c + 1) * head_width] - top) * factor)
                for c in range(repeat)
            ]
            page_sum = pieces[0]
            for piece in pieces[1:]:
                page_sum = page_sum + piece
            weights = jnp.concatenate([piece.astype(jnp.bfloat16) for piece in pieces], axis=1)
            at = pl.ds(pl.multiple_of(page * rows, rows), rows)
            s_buf[page, 0] = top
            s_buf[page, 1] = page_sum
            s_buf[page, 2] = jnp.dot(weights, v_buf[at, :], preferred_element_type=jnp.float32)
            highest = tuple(
                jnp.maximum(highest[r], jnp.where(owner == r, top, LOWEST)) for r in range(requests)
            )
        return highest

    local_max = lax.fori_loop(0, steps, attend, (lowest,) * requests)
    for r in range(requests):
        m_buf[r] = local_max[r]

    def combine(i, so_far):
        sums, outs = so_far
        for j in range(unroll):
            page = i * unroll + j
            owner = owner_of(page)
            lift = jnp.exp2((s_buf[page, 0] - m_buf[owner]) * factor)
            page_sum = lift * s_buf[page, 1]
            page_out = lift * s_buf[page, 2]
            sums = tuple(sums[r] + jnp.where(owner == r, page_sum, 0.0) for r in range(requests))
            outs = tuple(outs[r] + jnp.where(owner == r, page_out, 0.0) for r in range(requests))
        return sums, outs

    zero = jnp.zeros((query_heads, head_width), jnp.float32)
    sums, outs = lax.fori_loop(0, steps, combine, ((zero,) * requests, (zero,) * requests))

    low_lanes = lax.broadcasted_iota(jnp.int32, zero.shape, 1) < head_width // 2
    for r in range(requests):
        local_sum = jnp.broadcast_to(jnp.sum(sums[r], axis=1, keepdims=True), zero.shape)
        stats = jnp.where(low_lanes, local_max[r], local_sum)
        for half in range(subs):
            part = slice(half * own_heads, (half + 1) * own_heads)
            send[half, r] = outs[r][part]
            send[half, requests + r] = stats[part]

    copies = []
    for k in range(1, n):
        other_seq, other_sub = peer(k)
        copies.append(pltpu.make_async_remote_copy(
            src_ref=send.at[other_sub], dst_ref=recv.at[k - 1], send_sem=send_sems.at[k - 1],
            recv_sem=recv_sems.at[k - 1], device_id={"seq": other_seq, "sub": other_sub},
            device_id_type=MESH,
        ))
        copies[-1].start()
    for copy in copies:
        copy.wait_recv()

    half_width = head_width // 2
    for r in range(requests):
        parts = [(send[sub, requests + r], send[sub, r])]
        for k in range(n - 1):
            parts.append((recv[k, requests + r], recv[k, r]))
        top = parts[0][0]
        for stats, _ in parts[1:]:
            top = jnp.maximum(top, stats)
        top = top[:, :1]
        denominator = jnp.zeros((own_heads, 1), jnp.float32)
        numerator = jnp.zeros((own_heads, head_width), jnp.float32)
        for stats, out in parts:
            lift = jnp.exp2((stats[:, :1] - top) * factor)
            denominator = denominator + lift * stats[:, half_width:half_width + 1]
            numerator = numerator + lift * out
        out_ref[r] = (numerator / denominator).astype(out_ref.dtype)
    for copy in copies:
        copy.wait_send()


def shards(seqs, subs, queries, lengths, k_cache, v_cache):
    tokens, key_heads, head_width = k_cache.shape
    own_requests, query_heads, _ = queries.shape
    group_size = query_heads // key_heads
    requests = own_requests * subs
    pages = tokens // PAGE
    unroll = math.gcd(16, pages)
    steps = pages // unroll
    rows = PAGE * key_heads
    n = seqs * subs
    own_heads = query_heads // subs
    anywhere = pl.BlockSpec(memory_space=pltpu.HBM)
    sems = pltpu.SemaphoreType.DMA
    return pl.pallas_call(
        functools.partial(
            kernel, n, subs, pages, unroll, key_heads, own_requests, group_size, head_width
        ),
        out_shape=jax.ShapeDtypeStruct((requests, own_heads, head_width), jnp.bfloat16),
        in_specs=[anywhere] * 4,
        out_specs=pl.BlockSpec(memory_space=pltpu.VMEM),
        scratch_shapes=[
            pltpu.VMEM((subs, own_requests, query_heads, head_width), jnp.bfloat16),
            pltpu.SMEM((subs, 1, own_requests), jnp.int32),
            pltpu.VMEM((tokens * key_heads, head_width), jnp.bfloat16),
            pltpu.VMEM((tokens * key_heads, head_width), jnp.bfloat16),
            pltpu.VMEM((pages, 3, query_heads, head_width), jnp.float32),
            pltpu.VMEM((requests, query_heads, head_width), jnp.float32),
            pltpu.VMEM((subs, 2 * requests, own_heads, head_width), jnp.float32),
            pltpu.VMEM((n - 1, 2 * requests, own_heads, head_width), jnp.float32),
            sems((2 * subs - 1,)),
            sems((2 * subs - 1,)),
            sems((steps,)),
            sems((steps,)),
            sems((n - 1,)),
            sems((n - 1,)),
        ],
        compiler_params=pltpu.CompilerParams(
            collective_id=0, has_side_effects=True, vmem_limit_bytes=63 * 1024 * 1024
        ),
    )(
        queries,
        lengths.reshape(1, own_requests),
        k_cache.reshape(tokens * key_heads, head_width),
        v_cache.reshape(tokens * key_heads, head_width),
    )


def solution(mesh):
    return jax.shard_map(
        functools.partial(shards, mesh.shape["seq"], mesh.shape["sub"]),
        mesh=mesh,
        in_specs=(
            P(("group", "sub"), "head", None),
            P(("group", "sub")),
            P(("group", "seq", "sub"), "head", None),
            P(("group", "seq", "sub"), "head", None),
        ),
        out_specs=P("group", ("head", "sub"), None),
        check_vma=False,
    )
```
